32 devices in a mesh: section: 8 (over y, x, core), tp: 4 (over z).
Axes of the slice: x: 2, y: 2, z: 4, core: 2. Of those that a mesh axis runs over, the one named last changes fastest.
Arguments:
- stash: bfloat16 [8, 2, 256, 4096], P('section', None, 'tp'), may hold values from -660 to 660
- slot: int32 [8], P('section'), may hold values from 0 to 1
- doc_ids: int32 [8, 2, 256], P('section', None, 'tp'), may hold values from 0 to 3, never falling along the last dimension, each value on 1 to 128 neighbouring positions
- norm_gain: bfloat16 [4096], replicated, may hold values from 0.099609375 to 1.8984375
- w_query: bfloat16 [4096, 4096], P(None, 'tp'), may hold values from -21 to 21
- w_key: bfloat16 [4096, 1024], P(None, 'tp'), may hold values from -21 to 21
- value_weight: bfloat16 [4096, 1024], P(None, 'tp'), may hold values from -0.09375 to 0.09375
Outputs:
- received: bfloat16 [8, 256, 4096], P('section', None, 'tp')
The draws below stay inside these ranges and needn't reach their ends.
Inputs may be any that keep to these rules, and one draw needn't show every extreme that they name: `doc_ids`: document numbers never fall along a micro-batch.
All inputs are finite; a program needn't handle non-finite values.
Results may differ from the reference program's by a relative error of at most 0.025.
The reference program's roundings to bfloat16 on the way (of `picked`, `normed`, `values`, `softmax_weights` and `context`) count: a program that leaves them out, or rounds other values in their place, can miss the bound.
Values may be sent and summed in bfloat16 or wider, within the bound.
A program may use at most 64 MiB of HBM per device.

```python
import math
import jax
import jax.numpy as jnp
import numpy as np
from jax import lax

MODEL_WIDTH = 4096
HQ = 32
VALUE_KEY_HEADS = 8
HEAD_SIZE = 128
SLOTS = 2
DOCS = 4
TOK = 256
SECTIONS = 8


def weight_with_spike(key, salt_value, columns):
    gaussian = jax.random.truncated_normal(jax.random.fold_in(key, salt_value), -4.0, 4.0, (MODEL_WIDTH, columns), jnp.float32)
    gaussian = gaussian / jnp.sqrt(jnp.float32(MODEL_WIDTH))
    return gaussian.astype(jnp.bfloat16)


def draw_w_query(key, part):
    return weight_with_spike(key, 1, HQ * HEAD_SIZE)


def draw_w_key(key, part):
    return weight_with_spike(key, 2, VALUE_KEY_HEADS * HEAD_SIZE)


def draw_stash(key, part):
    full_shape = (SECTIONS, SLOTS, TOK, MODEL_WIDTH)
    col_scale = jnp.exp(jax.random.uniform(jax.random.fold_in(key, 12), (MODEL_WIDTH,), jnp.float32, 0.0, math.log(10.0)))
    row_scale = jnp.exp(jax.random.uniform(jax.random.fold_in(key, 11), (SECTIONS, SLOTS, TOK, 1), jnp.float32, 0.0, math.log(10.0)))
    noise_part = jax.random.truncated_normal(jax.random.fold_in(key, 13), -4.0, 4.0, full_shape, jnp.float32)
    result = noise_part * row_scale * col_scale
    return result.astype(jnp.bfloat16)


def place_ends(values, rng, low, largest):
    dims = values.shape
    spot = [jax.random.randint(jax.random.fold_in(rng, axis), (), 0, dims[axis]) for axis in range(len(dims))]
    values = values.at[tuple(spot)].set(low)
    longest = dims.index(max(dims))
    spot[longest] = (spot[longest] + 1) % dims[longest]
    return values.at[tuple(spot)].set(largest)


def block_levels(key, extent, cuts, least, largest):
    level, own = 1.0, jax.random.fold_in(key, 6)
    for position, shards_of in cuts:
        steps = jnp.exp(jax.random.uniform(jax.random.fold_in(own, position), (shards_of,), jnp.float32, least / len(cuts), largest / len(cuts)))
        level = level * jnp.repeat(steps, extent[position] // shards_of).reshape([-1 if axis == position else 1 for axis in range(len(extent))])
    return level


def length_profile(amount, total, bound, slope):
    loads = [(1 << 20) // math.isqrt(grade ** slope) + 1 for grade in range(2, amount + 1)]
    rest, holding = total - bound - (amount - 1), [1] * (amount - 1)
    while rest > 0:
        movable = [i for i in range(amount - 1) if holding[i] < bound]
        mass, remaining = sum([loads[i] for i in movable]), rest
        for i in movable:
            extra = min(bound - holding[i], max(1, remaining * loads[i] // mass), rest)
            holding[i] = holding[i] + extra
            rest = rest - extra
    return np.array([bound] + holding)


def ragged(key, count, total, most, lean):
    if count == 2:
        one = jax.random.randint(key, (), max(1, total - most), min(most, total - 1) + 1)
        return jnp.stack([one, total - one])
    tallies = jnp.asarray(length_profile(count, total, most, lean), jnp.int32)
    pairs = (count - 1) // 2
    donor, receiver = tallies[1:1 + 2 * pairs:2], tallies[2:2 + 2 * pairs:2]
    slack = jnp.minimum(donor - 1, most - receiver)
    moved = jax.random.randint(jax.random.fold_in(key, 1), (pairs,), 0, 1 << 20) % (slack + 1)
    tallies = tallies.at[1:1 + 2 * pairs:2].set(donor - moved).at[2:2 + 2 * pairs:2].set(receiver + moved)
    return tallies[jax.random.permutation(jax.random.fold_in(key, 2), count)]


def noise(stream_key, extent, width, most, split=(), kind=jnp.bfloat16):
    entries = jax.random.normal(stream_key, extent, jnp.float32) * width
    if len(split) > 0:
        entries = block_levels(stream_key, extent, split, -0.22, 0.18) * entries
    return jnp.clip(entries, min=-most, max=most).astype(kind)


def setup_inputs(seed: int = 0) -> dict:
    splits = jax.random.split(jax.random.key(seed), 8)
    stash = draw_stash(jax.random.fold_in(splits[7], 71), 0)
    slot = place_ends(jax.random.randint(splits[1], (SECTIONS,), 0, SLOTS), jax.random.fold_in(splits[1], 1), 0, SLOTS - 1).astype(jnp.int32)
    doc_ids = jax.vmap(lambda own: jnp.searchsorted(jnp.cumsum(ragged(own, DOCS, TOK, TOK // 2, 1)), jnp.arange(TOK), side="right"))(jax.random.split(splits[2], SECTIONS * SLOTS)).reshape((SECTIONS, SLOTS, TOK)).astype(jnp.int32)
    norm_gain = jnp.clip(1.0 + 0.18 * jax.random.normal(splits[3], (MODEL_WIDTH,), jnp.float32), 0.099609375, 1.8984375).astype(jnp.bfloat16)
    w_query = draw_w_query(jax.random.fold_in(splits[7], 71), 0)
    w_key = draw_w_key(jax.random.fold_in(splits[7], 71), 0)
    value_weight = noise(splits[6], (MODEL_WIDTH, VALUE_KEY_HEADS * HEAD_SIZE), MODEL_WIDTH ** -0.5, 0.09375, ((1, 4),))
    return dict(stash=stash, slot=slot, doc_ids=doc_ids, norm_gain=norm_gain, w_query=w_query, w_key=w_key, value_weight=value_weight)


ROPE_BASE = 500000.0
NORM_EPSILON = 1e-05

def rotate(values, positions):
    head_width = values.shape[-1]
    half_width = head_width // 2
    freq_index = jnp.arange(half_width, dtype=jnp.float32)
    inverse = jnp.power(jnp.float32(ROPE_BASE), -2.0 * freq_index / head_width)
    angles = positions.astype(jnp.float32)[:, None] * inverse[None, :]
    cosine = jnp.concatenate([jnp.cos(angles), jnp.cos(angles)], -1)[:, None, :]
    sine_part = jnp.concatenate([jnp.sin(angles), jnp.sin(angles)], -1)[:, None, :]
    turned = jnp.concatenate([-values[..., half_width:], values[..., :half_width]], -1)
    return values * cosine + turned * sine_part

def normalize(stash_rows, norm_gain):
    widened = stash_rows.astype(jnp.float32)
    mean_square = lax.optimization_barrier(jnp.mean(widened * widened, axis=-1, keepdims=True))
    return (widened * lax.rsqrt(mean_square + NORM_EPSILON) * norm_gain.astype(jnp.float32)).astype(jnp.bfloat16)

def project(normed, weight, positions, use_rope):
    length = normed.shape[0]
    product = jnp.dot(normed, weight, preferred_element_type=jnp.float32)
    if use_rope:
        product = rotate(product.reshape(length, -1, HEAD_SIZE), positions).reshape(length, -1)
    return product.astype(jnp.bfloat16)

def attend(queries, keys, values, doc_rows):
    length = queries.shape[0]
    kv_count = keys.shape[1] // HEAD_SIZE
    group_size = queries.shape[1] // HEAD_SIZE // kv_count
    grouped = queries.astype(jnp.float32).reshape(length, kv_count, group_size, HEAD_SIZE)
    key_heads = keys.astype(jnp.float32).reshape(length, kv_count, HEAD_SIZE)
    value_heads = values.astype(jnp.float32).reshape(length, kv_count, HEAD_SIZE)
    scores = jnp.einsum('ihgd,jhd->hgij', grouped, key_heads) * (1.0 / math.sqrt(HEAD_SIZE))
    row_index = jnp.arange(length, dtype=jnp.int32)[:, None]
    col_index = jnp.arange(length, dtype=jnp.int32)[None, :]
    allowed = (col_index <= row_index) & (doc_rows[None, :] == doc_rows[:, None])
    scores = jnp.where(allowed, scores, -1e+30)
    row_max = lax.optimization_barrier(jnp.max(scores, axis=-1, keepdims=True))
    score_exponent = jnp.exp(scores - row_max)
    softmax_weights = (score_exponent / lax.optimization_barrier(jnp.sum(score_exponent, axis=-1, keepdims=True))).astype(jnp.bfloat16)
    context = jnp.einsum('hgij,jhd->ihgd', softmax_weights.astype(jnp.float32), value_heads)
    return context.reshape(length, -1).astype(jnp.bfloat16)

def reference(stash, slot, doc_ids, norm_gain, w_query, w_key, value_weight):
    positions = jnp.arange(TOK, dtype=jnp.int32)

    def one_section(inputs):
        section_stash, section_slot, section_docs = inputs
        picked = lax.dynamic_index_in_dim(section_stash, section_slot, 0, keepdims=False)
        doc_rows = lax.dynamic_index_in_dim(section_docs, section_slot, 0, keepdims=False)
        normed = normalize(picked, norm_gain)
        queries = project(normed, w_query, positions, True)
        keys = project(normed, w_key, positions, True)
        values = project(normed, value_weight, positions, False)
        return attend(queries, keys, values, doc_rows)
    context_rows = lax.map(one_section, (stash, slot, doc_ids))
    return jnp.concatenate([jnp.zeros_like(context_rows[:1]), context_rows[:-1]], 0)
```

```python
import functools
import math

import jax
import jax.numpy as jnp
import numpy as np
from jax import lax
from jax.experimental import pallas as pl
from jax.experimental.pallas import tpu as pltpu
from jax.sharding import PartitionSpec as P

HEAD_SIZE = 128
ROPE_BASE = 500000.0
NORM_EPSILON = 1e-05
PIECES = 4
MESH = pl.DeviceIdType.MESH
ANY = pl.BlockSpec(memory_space=pl.ANY)
VMEM = pl.BlockSpec(memory_space=pltpu.VMEM)


def rope_tables(length):
    half = HEAD_SIZE // 2
    freq = np.arange(half, dtype=np.float32)
    inverse = np.power(np.float32(ROPE_BASE), np.float32(-2.0) * freq / np.float32(HEAD_SIZE)).astype(np.float32)
    angles = np.arange(length, dtype=np.float32)[:, None] * inverse[None, :]
    cos, sin = np.cos(angles), np.sin(angles)
    return (
        np.concatenate([cos, cos], -1).astype(np.float32),
        np.concatenate([-sin, sin], -1).astype(np.float32),
    )


def kernel(
    n, ns,
    slot_ref, stash_ref, doc_ref, gain_ref, cos_ref, sin_ref, wq_ref, wk_ref, wv_ref,
    out_ref,
    raw, mine, dmine, w, xbuf, dbuf, dcol, acc, q, k, v,
    raw_sem, w_sem, shift_send, right_send, left_send, recv,
    dshift_send, dright_send, dleft_send, drecv,
):
    me = lax.axis_index("tp")
    sec = lax.axis_index("section")
    slots, rows, width = raw.shape
    pieces = PIECES
    part = width // pieces
    nq, nk = wq_ref.shape[1], wk_ref.shape[1]
    total_n = w.shape[2]
    total = n * rows
    has_right, has_left = me + 1 < n, me > 0
    has_next, has_prev = sec + 1 < ns, sec > 0

    raw_copy = pltpu.make_async_copy(stash_ref.at[0], raw, raw_sem)
    raw_copy.start()

    bar = pltpu.get_barrier_semaphore()
    for cond, target in (
        (has_right, {"tp": me + 1}),
        (has_left, {"tp": me - 1}),
        (has_next, {"section": sec + 1}),
        (has_prev, {"section": sec - 1}),
    ):
        @pl.when(cond)
        def _():
            pl.semaphore_signal(bar, inc=1, device_id=target, device_id_type=MESH)

    def w_copies(p):
        span = pl.ds(pl.multiple_of(p * part, part), part)
        return (
            pltpu.make_async_copy(wq_ref.at[span], w.at[p, :, 0:nq], w_sem.at[p, 0]),
            pltpu.make_async_copy(wk_ref.at[span], w.at[p, :, nq:nq + nk], w_sem.at[p, 1]),
            pltpu.make_async_copy(wv_ref.at[span], w.at[p, :, nq + nk:total_n], w_sem.at[p, 2]),
        )

    @pl.when(has_prev)
    def _():
        for p in range(pieces):
            for c in w_copies(p):
                c.start()

    chosen = slot_ref[0]
    dmine[...] = jnp.zeros_like(dmine)
    docs = doc_ref[0, 0:1, :]
    for i in range(1, slots):
        docs = jnp.where(jnp.full(docs.shape, chosen, jnp.int32) == i, doc_ref[0, i:i + 1, :], docs)
    dmine[0:1, 0:rows] = docs
    raw_copy.wait()
    step = 16
    for r in range(0, rows, step):
        x = raw[0, r:r + step, :]
        for i in range(1, slots):
            x = jnp.where(jnp.full(x.shape, chosen, jnp.int32) == i, raw[i, r:r + step, :], x)
        x = x.astype(jnp.float32)
        scale = lax.rsqrt(jnp.mean(x * x, axis=-1, keepdims=True) + NORM_EPSILON)
        y = (x * scale * gain_ref[...].astype(jnp.float32)).astype(jnp.bfloat16)
        for p in range(pieces):
            mine[p, r:r + step, :] = y[:, p * part:(p + 1) * part]

    def edges(a):
        return a.astype(jnp.int32)

    pl.semaphore_wait(bar, edges(has_right) + edges(has_left) + edges(has_next) + edges(has_prev))

    def remote(src, dst, ss, rs, target):
        return pltpu.make_async_remote_copy(
            src_ref=src, dst_ref=dst, send_sem=ss, recv_sem=rs, device_id=target, device_id_type=MESH
        )

    def shift(p):
        return remote(mine.at[p], xbuf.at[me, p], shift_send.at[p], recv.at[me, p], {"section": sec + 1})

    def dshift():
        return remote(dmine, dbuf.at[me], dshift_send, drecv.at[me], {"section": sec + 1})

    def right(c, p):
        b = xbuf.at[c, p]
        return remote(b, b, right_send.at[c, p], recv.at[c, p], {"tp": me + 1})

    def left(c, p):
        b = xbuf.at[c, p]
        return remote(b, b, left_send.at[c, p], recv.at[c, p], {"tp": me - 1})

    def dright(c):
        b = dbuf.at[c]
        return remote(b, b, dright_send.at[c], drecv.at[c], {"tp": me + 1})

    def dleft(c):
        b = dbuf.at[c]
        return remote(b, b, dleft_send.at[c], drecv.at[c], {"tp": me - 1})

    @pl.when(has_next)
    def _():
        dshift().start()
        for p in range(pieces):
            shift(p).start()

    tile = 256

    def compute(c, p):
        x = xbuf[c, p]
        for t in range(0, total_n, tile):
            acc[c, :, t:t + tile] += jnp.dot(x, w[p, :, t:t + tile], preferred_element_type=jnp.float32)

        @pl.when(p == pieces - 1)
        def _():
            span = pl.ds(pl.multiple_of(c * rows, rows), rows)
            cos, sin = cos_ref[span, :], sin_ref[span, :]
            for h in range(0, nq + nk, HEAD_SIZE):
                u = acc[c, :, h:h + HEAD_SIZE]
                u = (u * cos + pltpu.roll(u, HEAD_SIZE // 2, 1) * sin).astype(jnp.bfloat16)
                if h < nq:
                    q[span, h:h + HEAD_SIZE] = u
                else:
                    k[span, h - nq:h - nq + HEAD_SIZE] = u
            v[span, :] = acc[c, :, nq + nk:total_n].astype(jnp.bfloat16)

    @pl.when(jnp.logical_not(has_prev))
    def _():
        out_ref[...] = jnp.zeros_like(out_ref)

    @pl.when(has_prev)
    def _():
        acc[...] = jnp.zeros_like(acc)


        dshift().wait_recv()

        @pl.when(has_right)
        def _():
            dright(me).start()

        @pl.when(has_left)
        def _():
            dleft(me).start()

        @pl.loop(0, pieces)
        def _(p):
            shift(p).wait_recv()

            @pl.when(has_right)
            def _():
                right(me, p).start()

            @pl.when(has_left)
            def _():
                left(me, p).start()

        @pl.loop(0, pieces)
        def _(p):
            for c in w_copies(p):
                c.wait()
            compute(me, p)

        @pl.loop(0, (n - 1) * pieces)
        def _(i):
            d, p = i // pieces + 1, i % pieces
            below, above = me - d, me + d

            @pl.when((below >= 0) & (p == 0))
            def _():
                dright(below).wait_recv()

                @pl.when(has_right)
                def _():
                    dright(below).start()

            @pl.when((above < n) & (p == 0))
            def _():
                dleft(above).wait_recv()

                @pl.when(has_left)
                def _():
                    dleft(above).start()

            @pl.when(below >= 0)
            def _():
                right(below, p).wait_recv()

                @pl.when(has_right)
                def _():
                    right(below, p).start()

            @pl.when(above < n)
            def _():
                left(above, p).wait_recv()

                @pl.when(has_left)
                def _():
                    left(above, p).start()

            @pl.when(below >= 0)
            def _():
                compute(below, p)

            @pl.when(above < n)
            def _():
                compute(above, p)

        pieces_row = [dbuf[c, 0:1, 0:rows] for c in range(n)]
        drow = jnp.concatenate(pieces_row, axis=1).astype(jnp.float32)
        lanes = dbuf.shape[2]
        for c in range(n):
            wide = jnp.broadcast_to(dbuf[c, 0:1, :].astype(jnp.float32), (lanes, lanes))
            dcol[c * rows:(c + 1) * rows, :] = wide.T[0:rows, :]

        group = (nq // HEAD_SIZE) // (nk // HEAD_SIZE)
        block = min(total, 256)
        factor = 1.0 / math.sqrt(HEAD_SIZE)
        for i in range(0, total, block):
            upto = i + block
            i_idx = lax.broadcasted_iota(jnp.int32, (block, upto), 0) + i
            j_idx = lax.broadcasted_iota(jnp.int32, (block, upto), 1)
            allowed = (j_idx <= i_idx) & (dcol[i:upto, 0:1] == drow[:, 0:upto])
            for h in range(nq // HEAD_SIZE):
                g = h // group
                scores = lax.dot_general(
                    q[i:upto, h * HEAD_SIZE:(h + 1) * HEAD_SIZE],
                    k[0:upto, g * HEAD_SIZE:(g + 1) * HEAD_SIZE],
                    (((1,), (1,)), ((), ())), preferred_element_type=jnp.float32,
                ) * factor
                scores = jnp.where(allowed, scores, -1e30)
                e = jnp.exp(scores - jnp.max(scores, axis=-1, keepdims=True))
                weights = (e * (1.0 / jnp.sum(e, axis=-1, keepdims=True))).astype(jnp.bfloat16)
                out_ref[0, i:upto, h * HEAD_SIZE:(h + 1) * HEAD_SIZE] = jnp.dot(
                    weights, v[0:upto, g * HEAD_SIZE:(g + 1) * HEAD_SIZE],
                    preferred_element_type=jnp.float32,
                ).astype(jnp.bfloat16)

        @pl.loop(0, n)
        def _(c):
            @pl.when(has_right & (c <= me))
            def _():
                dright(c).wait_send()
                for p in range(pieces):
                    right(c, p).wait_send()

            @pl.when(has_left & (c >= me))
            def _():
                dleft(c).wait_send()
                for p in range(pieces):
                    left(c, p).wait_send()

    @pl.when(has_next)
    def _():
        dshift().wait_send()
        for p in range(pieces):
            shift(p).wait_send()


def per_device(stash, slot, doc_ids, norm_gain, w_query, w_key, value_weight):
    n, ns = lax.axis_size("tp"), lax.axis_size("section")
    _, slots, rows, width = stash.shape
    total = n * rows
    nq, nk = w_query.shape[1], w_key.shape[1]
    total_n = nq + nk + value_weight.shape[1]
    cos, sin = rope_tables(total)
    lanes = -(-rows // 128) * 128
    bf, f32, dma = jnp.bfloat16, jnp.float32, pltpu.SemaphoreType.DMA
    part = width // PIECES
    return pl.pallas_call(
        functools.partial(kernel, n, ns),
        out_shape=jax.ShapeDtypeStruct((1, total, nq), bf),
        in_specs=[pl.BlockSpec(memory_space=pltpu.SMEM), ANY, VMEM, VMEM, VMEM, VMEM, ANY, ANY, ANY],
        out_specs=VMEM,
        scratch_shapes=[
            pltpu.VMEM((slots, rows, width), bf),
            pltpu.VMEM((PIECES, rows, part), bf),
            pltpu.VMEM((8, lanes), jnp.int32),
            pltpu.VMEM((PIECES, part, total_n), bf),
            pltpu.VMEM((n, PIECES, rows, part), bf),
            pltpu.VMEM((n, 8, lanes), jnp.int32),
            pltpu.VMEM((total, lanes), f32),
            pltpu.VMEM((n, rows, total_n), f32),
            pltpu.VMEM((total, nq), bf),
            pltpu.VMEM((total, nk), bf),
            pltpu.VMEM((total, nk), bf),
            dma,
            dma((PIECES, 3)),
            dma((PIECES,)),
            dma((n, PIECES)),
            dma((n, PIECES)),
            dma((n, PIECES)),
            dma,
            dma((n,)),
            dma((n,)),
            dma((n,)),
        ],
        compiler_params=pltpu.CompilerParams(collective_id=0, has_side_effects=True),
        cost_estimate=pl.CostEstimate(
            flops=2 * total * width * total_n, bytes_accessed=width * total_n * 2, transcendentals=0
        ),
    )(slot, stash, doc_ids, norm_gain[None], cos, sin, w_query, w_key, value_weight)


def solution(mesh):
    placed = (
        P("section", None, "tp", None),
        P("section"),
        P("section", None, "tp"),
        P(),
        P(None, "tp"),
        P(None, "tp"),
        P(None, "tp"),
    )
    return jax.shard_map(
        per_device, mesh=mesh, in_specs=placed, out_specs=P("section", None, "tp"), check_vma=False
    )
```

```python
import functools
import math

import jax
import jax.numpy as jnp
import numpy as np
from jax import lax
from jax.experimental import pallas as pl
from jax.experimental.pallas import tpu as pltpu
from jax.sharding import PartitionSpec as P

HEAD_SIZE = 128
ROPE_BASE = 500000.0
NORM_EPSILON = 1e-05
PIECES = 4
MESH = pl.DeviceIdType.MESH
ANY = pl.BlockSpec(memory_space=pl.ANY)
VMEM = pl.BlockSpec(memory_space=pltpu.VMEM)


def rope_tables(length):
    half = HEAD_SIZE // 2
    freq = np.arange(half, dtype=np.float32)
    inverse = np.power(np.float32(ROPE_BASE), np.float32(-2.0) * freq / np.float32(HEAD_SIZE)).astype(np.float32)
    angles = np.arange(length, dtype=np.float32)[:, None] * inverse[None, :]
    cos, sin = np.cos(angles), np.sin(angles)
    return (
        np.concatenate([cos, cos], -1).astype(np.float32),
        np.concatenate([-sin, sin], -1).astype(np.float32),
    )


def early_pieces(sec, ns):
    pairs = ns // 2
    count = PIECES * jnp.maximum(pairs - 1 - sec // 2, 0) // pairs if pairs else 0 * sec
    return jnp.where((sec % 2 == 1) & (sec + 1 < ns), count, 0)


def kernel(
    n, ns,
    slot_ref, stash_ref, doc_ref, gain_ref, cos_ref, sin_ref, wq_ref, wk_ref, wv_ref,
    q, k, v, dcol, drow,
    raw, mine, dmine, w, xbuf, zbuf, dbuf, acc,
    raw_sem, w_sem, shift_send, right_send, left_send, recv,
    zright_send, zleft_send, zrecv,
    dshift_send, dright_send, dleft_send, drecv,
):
    me = lax.axis_index("tp")
    sec = lax.axis_index("section")
    slots, rows, width = raw.shape
    pieces = PIECES
    part = width // pieces
    nq, nk = wq_ref.shape[1], wk_ref.shape[1]
    total_n = w.shape[2]
    total = n * rows
    has_right, has_left = me + 1 < n, me > 0
    has_next, has_prev = sec + 1 < ns, sec > 0
    early, early_prev = early_pieces(sec, ns), early_pieces(sec - 1, ns)

    raw_copy = pltpu.make_async_copy(stash_ref.at[0], raw, raw_sem)
    raw_copy.start()

    bar = pltpu.get_barrier_semaphore()
    for cond, target in (
        (has_right, {"tp": me + 1}),
        (has_left, {"tp": me - 1}),
        (has_next, {"section": sec + 1}),
        (has_prev, {"section": sec - 1}),
    ):
        @pl.when(cond)
        def _():
            pl.semaphore_signal(bar, inc=1, device_id=target, device_id_type=MESH)

    def w_copies(p):
        span = pl.ds(pl.multiple_of(p * part, part), part)
        return (
            pltpu.make_async_copy(wq_ref.at[span], w.at[p, :, 0:nq], w_sem.at[p, 0]),
            pltpu.make_async_copy(wk_ref.at[span], w.at[p, :, nq:nq + nk], w_sem.at[p, 1]),
            pltpu.make_async_copy(wv_ref.at[span], w.at[p, :, nq + nk:total_n], w_sem.at[p, 2]),
        )

    @pl.when(has_prev)
    def _():
        for p in range(pieces):
            for c in w_copies(p):
                c.start()

    chosen = slot_ref[0]
    dmine[...] = jnp.zeros_like(dmine)
    docs = doc_ref[0, 0:1, :]
    for i in range(1, slots):
        docs = jnp.where(jnp.full(docs.shape, chosen, jnp.int32) == i, doc_ref[0, i:i + 1, :], docs)
    dmine[0:1, 0:rows] = docs
    raw_copy.wait()
    step = 16
    for r in range(0, rows, step):
        x = raw[0, r:r + step, :]
        for i in range(1, slots):
            x = jnp.where(jnp.full(x.shape, chosen, jnp.int32) == i, raw[i, r:r + step, :], x)
        x = x.astype(jnp.float32)
        scale = lax.rsqrt(jnp.mean(x * x, axis=-1, keepdims=True) + NORM_EPSILON)
        y = (x * scale * gain_ref[...].astype(jnp.float32)[None, :]).astype(jnp.bfloat16)
        for p in range(pieces):
            mine[p, r:r + step, :] = y[:, p * part:(p + 1) * part]

    def edges(a):
        return a.astype(jnp.int32)

    pl.semaphore_wait(bar, edges(has_right) + edges(has_left) + edges(has_next) + edges(has_prev))

    def remote(src, dst, ss, rs, target):
        return pltpu.make_async_remote_copy(
            src_ref=src, dst_ref=dst, send_sem=ss, recv_sem=rs, device_id=target, device_id_type=MESH
        )

    def hop(src, c, p):
        return remote(src, xbuf.at[c, p], shift_send.at[c, p], recv.at[c, p], {"section": sec + 1})

    def shift(p):
        return hop(mine.at[p], me, p)

    def zright(src, c, p):
        return remote(src, zbuf.at[c, p], zright_send.at[c, p], zrecv.at[c, p], {"tp": me + 1})

    def zleft(src, c, p):
        return remote(src, zbuf.at[c, p], zleft_send.at[c, p], zrecv.at[c, p], {"tp": me - 1})

    def dshift():
        return remote(dmine, dbuf.at[me], dshift_send, drecv.at[me], {"section": sec + 1})

    def right(c, p):
        b = xbuf.at[c, p]
        return remote(b, b, right_send.at[c, p], recv.at[c, p], {"tp": me + 1})

    def left(c, p):
        b = xbuf.at[c, p]
        return remote(b, b, left_send.at[c, p], recv.at[c, p], {"tp": me - 1})

    def dright(c):
        b = dbuf.at[c]
        return remote(b, b, dright_send.at[c], drecv.at[c], {"tp": me + 1})

    def dleft(c):
        b = dbuf.at[c]
        return remote(b, b, dleft_send.at[c], drecv.at[c], {"tp": me - 1})

    @pl.when(has_next)
    def _():
        dshift().start()
        for p in range(pieces):
            shift(p).start()
            for cond, make in ((has_right, zright), (has_left, zleft)):
                @pl.when(cond & (p < early))
                def _():
                    make(mine.at[p], me, p).start()

    tile = 256

    def compute(c, p, last):
        x = xbuf[c, p]
        for t in range(0, total_n, tile):
            acc[c, :, t:t + tile] += jnp.dot(x, w[p, :, t:t + tile], preferred_element_type=jnp.float32)

        @pl.when(last)
        def _():
            span = pl.ds(pl.multiple_of(c * rows, rows), rows)
            cos, sin = cos_ref[span, :], sin_ref[span, :]
            for h in range(0, nq + nk, HEAD_SIZE):
                u = acc[c, :, h:h + HEAD_SIZE]
                u = (u * cos + pltpu.roll(u, HEAD_SIZE // 2, 1) * sin).astype(jnp.bfloat16)
                if h < nq:
                    q[span, h:h + HEAD_SIZE] = u
                else:
                    k[span, h - nq:h - nq + HEAD_SIZE] = u
            v[span, :] = acc[c, :, nq + nk:total_n].astype(jnp.bfloat16)

    def own_forward():
        @pl.loop(0, pieces)
        def _(p):
            @pl.when(has_right & (p >= early_prev))
            def _():
                right(me, p).start()

            @pl.when(has_left & (p >= early_prev))
            def _():
                left(me, p).start()

    def keep_docs(c):
        drow[c] = dbuf[c]
        lanes = dbuf.shape[2]
        wide = jnp.broadcast_to(dbuf[c, 0:1, :].astype(jnp.float32), (lanes, lanes))
        dcol[pl.ds(pl.multiple_of(c * rows, rows), rows), :] = wide.T[0:rows, :]

    @pl.when(has_prev)
    def _():
        acc[...] = jnp.zeros_like(acc)
        dshift().wait_recv()

        @pl.when(has_right)
        def _():
            dright(me).start()

        @pl.when(has_left)
        def _():
            dleft(me).start()

        keep_docs(me)

        @pl.loop(0, pieces)
        def _(p):
            shift(p).wait_recv()

        @pl.when(early == 0)
        def _():
            own_forward()

    @pl.loop(0, (n - 1) * pieces)
    def _(i):
        d, p = i // pieces + 1, i % pieces
        below, above = me - d, me + d
        valid = p < early

        @pl.when(valid & (below >= 0))
        def _():
            b = zbuf.at[below, p]
            zright(b, below, p).wait_recv()

            @pl.when(has_right)
            def _():
                zright(b, below, p).start()

            hop(b, below, p).start()

        @pl.when(valid & (above < n))
        def _():
            b = zbuf.at[above, p]
            zleft(b, above, p).wait_recv()

            @pl.when(has_left)
            def _():
                zleft(b, above, p).start()

            hop(b, above, p).start()

        @pl.when(has_prev & (i < pieces))
        def _():
            for c in w_copies(p):
                c.wait()
            compute(me, p, p == pieces - 1)

    @pl.when(has_prev)
    def _():
        @pl.when(early > 0)
        def _():
            own_forward()

        @pl.loop(0, (n - 1) * pieces)
        def _(i):
            d, p = i // pieces + 1, i % pieces
            below, above = me - d, me + d
            late = p >= early_prev

            @pl.when((below >= 0) & (p == 0))
            def _():
                dright(below).wait_recv()

                @pl.when(has_right)
                def _():
                    dright(below).start()

                keep_docs(below)

            @pl.when((above < n) & (p == 0))
            def _():
                dleft(above).wait_recv()

                @pl.when(has_left)
                def _():
                    dleft(above).start()

                keep_docs(above)

            @pl.when(late & (below >= 0))
            def _():
                right(below, p).wait_recv()

                @pl.when(has_right)
                def _():
                    right(below, p).start()

            @pl.when(late & (above < n))
            def _():
                left(above, p).wait_recv()

                @pl.when(has_left)
                def _():
                    left(above, p).start()

            last = (p == pieces - 1) & (early_prev == 0)

            @pl.when(late & (below >= 0))
            def _():
                compute(below, p, last)

            @pl.when(late & (above < n))
            def _():
                compute(above, p, last)

        @pl.loop(0, n * pieces)
        def _(i):
            c, p = i // pieces, i % pieces

            @pl.when((c != me) & (p < early_prev))
            def _():
                hop(xbuf.at[c, p], c, p).wait_recv()
                compute(c, p, p == early_prev - 1)

        @pl.loop(0, n * pieces)
        def _(i):
            c, p = i // pieces, i % pieces

            @pl.when(has_right & (c <= me) & (p == 0))
            def _():
                dright(c).wait_send()

            @pl.when(has_left & (c >= me) & (p == 0))
            def _():
                dleft(c).wait_send()

            @pl.when(has_right & (c <= me) & (p >= early_prev))
            def _():
                right(c, p).wait_send()

            @pl.when(has_left & (c >= me) & (p >= early_prev))
            def _():
                left(c, p).wait_send()

    @pl.when(has_next)
    def _():
        dshift().wait_send()

        @pl.loop(0, n * pieces)
        def _(i):
            c, p = i // pieces, i % pieces

            @pl.when((c == me) | (p < early))
            def _():
                hop(zbuf.at[c, p], c, p).wait_send()

            @pl.when(has_right & (c <= me) & (p < early))
            def _():
                zright(zbuf.at[c, p], c, p).wait_send()

            @pl.when(has_left & (c >= me) & (p < early))
            def _():
                zleft(zbuf.at[c, p], c, p).wait_send()


def attend(n, rows, q, k, v, dcol, drow, out_ref):
    sec = lax.axis_index("section")
    g = pl.program_id(0)
    total = n * rows
    group = out_ref.shape[2] // HEAD_SIZE
    block = 128 if total % 128 == 0 else total
    factor = 1.0 / math.sqrt(HEAD_SIZE)

    @pl.when(sec == 0)
    def _():
        out_ref[...] = jnp.zeros_like(out_ref)

    @pl.when(sec > 0)
    def _():
        lane_docs = jnp.concatenate([drow[c, 0:1, 0:rows] for c in range(n)], axis=1).astype(jnp.float32)
        cols = pl.ds(pl.multiple_of(g * HEAD_SIZE, HEAD_SIZE), HEAD_SIZE)
        for i in range(0, total, block):
            upto = i + block
            i_idx = lax.broadcasted_iota(jnp.int32, (block, upto), 0) + i
            j_idx = lax.broadcasted_iota(jnp.int32, (block, upto), 1)
            allowed = (j_idx <= i_idx) & (dcol[i:upto, 0:1] == lane_docs[:, 0:upto])
            for h in range(group):
                wide = pl.ds(pl.multiple_of((g * group + h) * HEAD_SIZE, HEAD_SIZE), HEAD_SIZE)
                scores = lax.dot_general(
                    q[i:upto, wide], k[0:upto, cols],
                    (((1,), (1,)), ((), ())), preferred_element_type=jnp.float32,
                ) * factor
                scores = jnp.where(allowed, scores, -1e30)
                e = jnp.exp(scores - jnp.max(scores, axis=-1, keepdims=True))
                weights = (e * (1.0 / jnp.sum(e, axis=-1, keepdims=True))).astype(jnp.bfloat16)
                out_ref[0, i:upto, h * HEAD_SIZE:(h + 1) * HEAD_SIZE] = jnp.dot(
                    weights, v[0:upto, cols], preferred_element_type=jnp.float32,
                ).astype(jnp.bfloat16)


def per_device(stash, slot, doc_ids, norm_gain, w_query, w_key, value_weight):
    n, ns = lax.axis_size("tp"), lax.axis_size("section")
    _, slots, rows, width = stash.shape
    total = n * rows
    nq, nk = w_query.shape[1], w_key.shape[1]
    total_n = nq + nk + value_weight.shape[1]
    cos, sin = rope_tables(total)
    lanes = -(-rows // 128) * 128
    bf, f32, dma = jnp.bfloat16, jnp.float32, pltpu.SemaphoreType.DMA
    part = width // PIECES
    q, k, v, dcol, drow = pl.pallas_call(
        functools.partial(kernel, n, ns),
        out_shape=(
            jax.ShapeDtypeStruct((total, nq), bf),
            jax.ShapeDtypeStruct((total, nk), bf),
            jax.ShapeDtypeStruct((total, nk), bf),
            jax.ShapeDtypeStruct((total, lanes), f32),
            jax.ShapeDtypeStruct((n, 8, lanes), jnp.int32),
        ),
        in_specs=[pl.BlockSpec(memory_space=pltpu.SMEM), ANY, VMEM, VMEM, VMEM, VMEM, ANY, ANY, ANY],
        out_specs=(VMEM,) * 5,
        scratch_shapes=[
            pltpu.VMEM((slots, rows, width), bf),
            pltpu.VMEM((PIECES, rows, part), bf),
            pltpu.VMEM((8, lanes), jnp.int32),
            pltpu.VMEM((PIECES, part, total_n), bf),
            pltpu.VMEM((n, PIECES, rows, part), bf),
            pltpu.VMEM((n, PIECES, rows, part), bf),
            pltpu.VMEM((n, 8, lanes), jnp.int32),
            pltpu.VMEM((n, rows, total_n), f32),
            dma,
            dma((PIECES, 3)),
            dma((n, PIECES)),
            dma((n, PIECES)),
            dma((n, PIECES)),
            dma((n, PIECES)),
            dma((n, PIECES)),
            dma((n, PIECES)),
            dma((n, PIECES)),
            dma,
            dma((n,)),
            dma((n,)),
            dma((n,)),
        ],
        compiler_params=pltpu.CompilerParams(collective_id=0, has_side_effects=True),
        cost_estimate=pl.CostEstimate(
            flops=2 * total * width * total_n, bytes_accessed=width * total_n * 2, transcendentals=0
        ),
    )(slot, stash, doc_ids, norm_gain, cos, sin, w_query, w_key, value_weight)
    heads = nk // HEAD_SIZE
    return pl.pallas_call(
        functools.partial(attend, n, rows),
        grid=(heads,),
        out_shape=jax.ShapeDtypeStruct((1, total, nq), bf),
        in_specs=[VMEM] * 5,
        out_specs=pl.BlockSpec((1, total, nq // heads), lambda g: (0, 0, g)),
    )(q, k, v, dcol, drow)


def solution(mesh):
    placed = (
        P("section", None, "tp", None),
        P("section"),
        P("section", None, "tp"),
        P(),
        P(None, "tp"),
        P(None, "tp"),
        P(None, "tp"),
    )
    return jax.shard_map(
        per_device, mesh=mesh, in_specs=placed, out_specs=P("section", None, "tp"), check_vma=False
    )
```

```python
import functools
import math

import jax
import jax.numpy as jnp
import numpy as np
from jax import lax
from jax.experimental import pallas as pl
from jax.experimental.pallas import tpu as pltpu
from jax.sharding import PartitionSpec as P

HEAD_SIZE = 128
ROPE_BASE = 500000.0
NORM_EPSILON = 1e-05
PIECES = 4
MESH = pl.DeviceIdType.MESH
GATHER_VMEM = 52 << 20
ATTEND_VMEM = 24 << 20
ANY = pl.BlockSpec(memory_space=pltpu.HBM)
VMEM = pl.BlockSpec(memory_space=pltpu.VMEM)


def rope_tables(length):
    half = HEAD_SIZE // 2
    freq = np.arange(half, dtype=np.float32)
    inverse = np.power(np.float32(ROPE_BASE), np.float32(-2.0) * freq / np.float32(HEAD_SIZE)).astype(np.float32)
    angles = np.arange(length, dtype=np.float32)[:, None] * inverse[None, :]
    cos, sin = np.cos(angles), np.sin(angles)
    return (
        np.concatenate([cos, cos], -1).astype(np.float32),
        np.concatenate([-sin, sin], -1).astype(np.float32),
    )


def early_pieces(sec, ns):
    pairs = ns // 2
    count = PIECES * jnp.maximum(pairs - 1 - sec // 2, 0) // pairs if pairs else 0 * sec
    return jnp.where((sec % 2 == 1) & (sec + 1 < ns), count, 0)


def kernel(
    n, ns,
    slot_ref, stash_ref, doc_ref, gain_ref, cos_ref, sin_ref, wq_ref, wk_ref, wv_ref,
    q, k, v, dcol, drow,
    raw, mine, dmine, w, xbuf, zbuf, dbuf, acc,
    raw_sem, w_sem, shift_send, right_send, left_send, recv,
    zright_send, zleft_send, zrecv,
    dshift_send, dright_send, dleft_send, drecv,
):
    me = lax.axis_index("tp")
    sec = lax.axis_index("section")
    slots, rows, width = raw.shape
    pieces = PIECES
    part = width // pieces
    nq, nk = wq_ref.shape[1], wk_ref.shape[1]
    total_n = w.shape[2]
    total = n * rows
    has_right, has_left = me + 1 < n, me > 0
    has_next, has_prev = sec + 1 < ns, sec > 0
    early, early_prev = early_pieces(sec, ns), early_pieces(sec - 1, ns)

    raw_copy = pltpu.make_async_copy(stash_ref.at[0], raw, raw_sem)
    raw_copy.start()

    bar = pltpu.get_barrier_semaphore()
    for cond, target in (
        (has_right, {"tp": me + 1}),
        (has_left, {"tp": me - 1}),
        (has_next, {"section": sec + 1}),
        (has_prev, {"section": sec - 1}),
    ):
        @pl.when(cond)
        def _():
            pl.semaphore_signal(bar, inc=1, device_id=target, device_id_type=MESH)

    def w_copies(p):
        span = pl.ds(pl.multiple_of(p * part, part), part)
        return (
            pltpu.make_async_copy(wq_ref.at[span], w.at[p, :, 0:nq], w_sem.at[p, 0]),
            pltpu.make_async_copy(wk_ref.at[span], w.at[p, :, nq:nq + nk], w_sem.at[p, 1]),
            pltpu.make_async_copy(wv_ref.at[span], w.at[p, :, nq + nk:total_n], w_sem.at[p, 2]),
        )

    @pl.when(has_prev)
    def _():
        for p in range(pieces):
            for c in w_copies(p):
                c.start()

    chosen = slot_ref[0]
    dmine[...] = jnp.zeros_like(dmine)
    docs = doc_ref[0, 0:1, :]
    for i in range(1, slots):
        docs = jnp.where(jnp.full(docs.shape, chosen, jnp.int32) == i, doc_ref[0, i:i + 1, :], docs)
    dmine[0:1, 0:rows] = docs
    raw_copy.wait()
    step = 16
    for r in range(0, rows, step):
        x = raw[0, r:r + step, :]
        for i in range(1, slots):
            x = jnp.where(jnp.full(x.shape, chosen, jnp.int32) == i, raw[i, r:r + step, :], x)
        x = x.astype(jnp.float32)
        scale = lax.rsqrt(jnp.mean(x * x, axis=-1, keepdims=True) + NORM_EPSILON)
        y = (x * scale * gain_ref[...].astype(jnp.float32)[None, :]).astype(jnp.bfloat16)
        for p in range(pieces):
            mine[p, r:r + step, :] = y[:, p * part:(p + 1) * part]

    def edges(a):
        return a.astype(jnp.int32)

    pl.semaphore_wait(bar, edges(has_right) + edges(has_left) + edges(has_next) + edges(has_prev))

    def remote(src, dst, ss, rs, target):
        return pltpu.make_async_remote_copy(
            src_ref=src, dst_ref=dst, send_sem=ss, recv_sem=rs, device_id=target, device_id_type=MESH
        )

    def hop(src, c, p):
        return remote(src, xbuf.at[c, p], shift_send.at[c, p], recv.at[c, p], {"section": sec + 1})

    def shift(p):
        return hop(mine.at[p], me, p)

    def zright(src, c, p):
        return remote(src, zbuf.at[c, p], zright_send.at[c, p], zrecv.at[c, p], {"tp": me + 1})

    def zleft(src, c, p):
        return remote(src, zbuf.at[c, p], zleft_send.at[c, p], zrecv.at[c, p], {"tp": me - 1})

    def dshift():
        return remote(dmine, dbuf.at[me], dshift_send, drecv.at[me], {"section": sec + 1})

    def right(c, p):
        b = xbuf.at[c, p]
        return remote(b, b, right_send.at[c, p], recv.at[c, p], {"tp": me + 1})

    def left(c, p):
        b = xbuf.at[c, p]
        return remote(b, b, left_send.at[c, p], recv.at[c, p], {"tp": me - 1})

    def dright(c):
        b = dbuf.at[c]
        return remote(b, b, dright_send.at[c], drecv.at[c], {"tp": me + 1})

    def dleft(c):
        b = dbuf.at[c]
        return remote(b, b, dleft_send.at[c], drecv.at[c], {"tp": me - 1})

    @pl.when(has_next)
    def _():
        dshift().start()
        for p in range(pieces):
            shift(p).start()
            for cond, make in ((has_right, zright), (has_left, zleft)):
                @pl.when(cond & (p < early))
                def _():
                    make(mine.at[p], me, p).start()

    tile = 256

    def compute(c, p, last):
        x = xbuf[c, p]
        for t in range(0, total_n, tile):
            acc[c, :, t:t + tile] += jnp.dot(x, w[p, :, t:t + tile], preferred_element_type=jnp.float32)

        @pl.when(last)
        def _():
            span = pl.ds(pl.multiple_of(c * rows, rows), rows)
            cos, sin = cos_ref[span, :], sin_ref[span, :]
            for h in range(0, nq + nk, HEAD_SIZE):
                u = acc[c, :, h:h + HEAD_SIZE]
                u = (u * cos + pltpu.roll(u, HEAD_SIZE // 2, 1) * sin).astype(jnp.bfloat16)
                if h < nq:
                    q[span, h:h + HEAD_SIZE] = u
                else:
                    k[span, h - nq:h - nq + HEAD_SIZE] = u
            v[span, :] = acc[c, :, nq + nk:total_n].astype(jnp.bfloat16)

    def own_forward():
        @pl.loop(0, pieces)
        def _(p):
            @pl.when(has_right & (p >= early_prev))
            def _():
                right(me, p).start()

            @pl.when(has_left & (p >= early_prev))
            def _():
                left(me, p).start()

    def keep_docs(c):
        drow[c] = dbuf[c]
        lanes = dbuf.shape[2]
        wide = jnp.broadcast_to(dbuf[c, 0:1, :].astype(jnp.float32), (lanes, lanes))
        dcol[pl.ds(pl.multiple_of(c * rows, rows), rows), :] = wide.T[0:rows, :]

    @pl.when(has_prev)
    def _():
        acc[...] = jnp.zeros_like(acc)
        dshift().wait_recv()

        @pl.when(has_right)
        def _():
            dright(me).start()

        @pl.when(has_left)
        def _():
            dleft(me).start()

        keep_docs(me)

        @pl.loop(0, pieces)
        def _(p):
            shift(p).wait_recv()

        own_forward()

        @pl.loop(0, pieces)
        def _(p):
            for c in w_copies(p):
                c.wait()
            compute(me, p, p == pieces - 1)

    def pass_early(d, p):
        below, above = me - d, me + d

        @pl.when(below >= 0)
        def _():
            b = zbuf.at[below, p]
            zright(b, below, p).wait_recv()

            @pl.when(has_right)
            def _():
                zright(b, below, p).start()

            hop(b, below, p).start()

        @pl.when(above < n)
        def _():
            b = zbuf.at[above, p]
            zleft(b, above, p).wait_recv()

            @pl.when(has_left)
            def _():
                zleft(b, above, p).start()

            hop(b, above, p).start()

    @pl.when(has_prev)
    def _():
        @pl.loop(0, (n - 1) * pieces)
        def _(i):
            d, p = i // pieces + 1, i % pieces
            below, above = me - d, me + d
            late = p >= early_prev

            @pl.when(p == 0)
            def _():
                @pl.loop(0, pieces)
                def _(e):
                    @pl.when(e < early)
                    def _():
                        pass_early(d, e)

            @pl.when((below >= 0) & (p == 0))
            def _():
                dright(below).wait_recv()

                @pl.when(has_right)
                def _():
                    dright(below).start()

                keep_docs(below)

            @pl.when((above < n) & (p == 0))
            def _():
                dleft(above).wait_recv()

                @pl.when(has_left)
                def _():
                    dleft(above).start()

                keep_docs(above)

            @pl.when(late & (below >= 0))
            def _():
                right(below, p).wait_recv()

                @pl.when(has_right)
                def _():
                    right(below, p).start()

            @pl.when(late & (above < n))
            def _():
                left(above, p).wait_recv()

                @pl.when(has_left)
                def _():
                    left(above, p).start()

            last = (p == pieces - 1) & (early_prev == 0)

            @pl.when(late & (below >= 0))
            def _():
                compute(below, p, last)

            @pl.when(late & (above < n))
            def _():
                compute(above, p, last)

        @pl.loop(0, n * pieces)
        def _(i):
            c, p = i // pieces, i % pieces

            @pl.when((c != me) & (p < early_prev))
            def _():
                hop(xbuf.at[c, p], c, p).wait_recv()
                compute(c, p, p == early_prev - 1)

        @pl.loop(0, n * pieces)
        def _(i):
            c, p = i // pieces, i % pieces

            @pl.when(has_right & (c <= me) & (p == 0))
            def _():
                dright(c).wait_send()

            @pl.when(has_left & (c >= me) & (p == 0))
            def _():
                dleft(c).wait_send()

            @pl.when(has_right & (c <= me) & (p >= early_prev))
            def _():
                right(c, p).wait_send()

            @pl.when(has_left & (c >= me) & (p >= early_prev))
            def _():
                left(c, p).wait_send()

    @pl.when(has_next)
    def _():
        dshift().wait_send()

        @pl.loop(0, n * pieces)
        def _(i):
            c, p = i // pieces, i % pieces

            @pl.when((c == me) | (p < early))
            def _():
                hop(zbuf.at[c, p], c, p).wait_send()

            @pl.when(has_right & (c <= me) & (p < early))
            def _():
                zright(zbuf.at[c, p], c, p).wait_send()

            @pl.when(has_left & (c >= me) & (p < early))
            def _():
                zleft(zbuf.at[c, p], c, p).wait_send()


def attend(n, rows, q, k, v, dcol, drow, out_ref, s_buf, p_buf):
    sec = lax.axis_index("section")
    g = pl.program_id(0)
    total = n * rows
    group = out_ref.shape[2] // HEAD_SIZE
    block = 128 if total % 128 == 0 else total
    factor = math.log2(math.e) / math.sqrt(HEAD_SIZE)

    @pl.when(sec == 0)
    def _():
        out_ref[...] = jnp.zeros_like(out_ref)

    @pl.when(sec > 0)
    def _():
        lane_docs = jnp.concatenate([drow[c, 0:1, 0:rows] for c in range(n)], axis=1).astype(jnp.float32)
        cols = pl.ds(pl.multiple_of(g * HEAD_SIZE, HEAD_SIZE), HEAD_SIZE)
        vg = v[:, cols]
        vg = jnp.concatenate([vg, jnp.ones_like(vg)], axis=1)
        starts = range(0, total, block)
        for i in starts:
            upto = i + block
            keys = k[0:upto, cols]
            i_idx = lax.broadcasted_iota(jnp.int32, (block, upto), 0) + i
            j_idx = lax.broadcasted_iota(jnp.int32, (block, upto), 1)
            allowed = (j_idx <= i_idx) & (dcol[i:upto, 0:1] == lane_docs[:, 0:upto])
            for h in range(group):
                wide = pl.ds(pl.multiple_of((g * group + h) * HEAD_SIZE, HEAD_SIZE), HEAD_SIZE)
                raw = lax.dot_general(
                    q[i:upto, wide], keys, (((1,), (1,)), ((), ())), preferred_element_type=jnp.float32
                )
                s_buf[h, i:upto, 0:upto] = jnp.where(allowed, raw, -1e30)
        for i in starts:
            upto = i + block
            for h in range(group):
                x = s_buf[h, i:upto, 0:upto]
                e = jnp.exp2((x - jnp.max(x, axis=-1, keepdims=True)) * factor)
                p_buf[h, i:upto, 0:upto] = e.astype(jnp.bfloat16)
        for i in starts:
            upto = i + block
            for h in range(group):
                both = jnp.dot(p_buf[h, i:upto, 0:upto], vg[0:upto], preferred_element_type=jnp.float32)
                out_ref[0, i:upto, h * HEAD_SIZE:(h + 1) * HEAD_SIZE] = (
                    both[:, 0:HEAD_SIZE] / both[:, HEAD_SIZE:]
                ).astype(jnp.bfloat16)


def per_device(stash, slot, doc_ids, norm_gain, w_query, w_key, value_weight):
    n, ns = lax.axis_size("tp"), lax.axis_size("section")
    _, slots, rows, width = stash.shape
    total = n * rows
    nq, nk = w_query.shape[1], w_key.shape[1]
    total_n = nq + nk + value_weight.shape[1]
    cos, sin = rope_tables(total)
    lanes = -(-rows // 128) * 128
    bf, f32, dma = jnp.bfloat16, jnp.float32, pltpu.SemaphoreType.DMA
    part = width // PIECES
    q, k, v, dcol, drow = pl.pallas_call(
        functools.partial(kernel, n, ns),
        out_shape=(
            jax.ShapeDtypeStruct((total, nq), bf),
            jax.ShapeDtypeStruct((total, nk), bf),
            jax.ShapeDtypeStruct((total, nk), bf),
            jax.ShapeDtypeStruct((total, lanes), f32),
            jax.ShapeDtypeStruct((n, 8, lanes), jnp.int32),
        ),
        in_specs=[pl.BlockSpec(memory_space=pltpu.SMEM), ANY, VMEM, VMEM, VMEM, VMEM, ANY, ANY, ANY],
        out_specs=(VMEM,) * 5,
        scratch_shapes=[
            pltpu.VMEM((slots, rows, width), bf),
            pltpu.VMEM((PIECES, rows, part), bf),
            pltpu.VMEM((8, lanes), jnp.int32),
            pltpu.VMEM((PIECES, part, total_n), bf),
            pltpu.VMEM((n, PIECES, rows, part), bf),
            pltpu.VMEM((n, PIECES, rows, part), bf),
            pltpu.VMEM((n, 8, lanes), jnp.int32),
            pltpu.VMEM((n, rows, total_n), f32),
            dma,
            dma((PIECES, 3)),
            dma((n, PIECES)),
            dma((n, PIECES)),
            dma((n, PIECES)),
            dma((n, PIECES)),
            dma((n, PIECES)),
            dma((n, PIECES)),
            dma((n, PIECES)),
            dma,
            dma((n,)),
            dma((n,)),
            dma((n,)),
        ],
        compiler_params=pltpu.CompilerParams(
            collective_id=0, has_side_effects=True, vmem_limit_bytes=GATHER_VMEM
        ),
        cost_estimate=pl.CostEstimate(
            flops=2 * total * width * total_n, bytes_accessed=width * total_n * 2, transcendentals=0
        ),
    )(slot, stash, doc_ids, norm_gain, cos, sin, w_query, w_key, value_weight)
    heads = nk // HEAD_SIZE
    return pl.pallas_call(
        functools.partial(attend, n, rows),
        grid=(heads,),
        out_shape=jax.ShapeDtypeStruct((1, total, nq), bf),
        in_specs=[VMEM] * 5,
        out_specs=pl.BlockSpec((1, total, nq // heads), lambda g: (0, 0, g)),
        scratch_shapes=[
            pltpu.VMEM((nq // nk, total, total), f32),
            pltpu.VMEM((nq // nk, total, total), bf),
        ],
        compiler_params=pltpu.CompilerParams(vmem_limit_bytes=ATTEND_VMEM),
    )(q, k, v, dcol, drow)


def solution(mesh):
    placed = (
        P("section", None, "tp", None),
        P("section"),
        P("section", None, "tp"),
        P(),
        P(None, "tp"),
        P(None, "tp"),
        P(None, "tp"),
    )
    return jax.shard_map(
        per_device, mesh=mesh, in_specs=placed, out_specs=P("section", None, "tp"), check_vma=False
    )
```

```python
import functools
import math

import jax
import jax.numpy as jnp
import numpy as np
from jax import lax
from jax.experimental import pallas as pl
from jax.experimental.pallas import tpu as pltpu
from jax.sharding import PartitionSpec as P

HEAD_SIZE = 128
ROPE_BASE = 500000.0
NORM_EPSILON = 1e-05
PIECES = 4
MESH = pl.DeviceIdType.MESH
GATHER_VMEM = 60 << 20
ATTEND_VMEM = 60 << 20
ANY = pl.BlockSpec(memory_space=pltpu.HBM)
VMEM = pl.BlockSpec(memory_space=pltpu.VMEM)


def rope_tables(length):
    half = HEAD_SIZE // 2
    freq = np.arange(half, dtype=np.float32)
    inverse = np.power(np.float32(ROPE_BASE), np.float32(-2.0) * freq / np.float32(HEAD_SIZE)).astype(np.float32)
    angles = np.arange(length, dtype=np.float32)[:, None] * inverse[None, :]
    cos, sin = np.cos(angles), np.sin(angles)
    return (
        np.concatenate([cos, cos], -1).astype(np.float32),
        np.concatenate([-sin, sin], -1).astype(np.float32),
    )


def early_pieces(sec, ns):
    pairs = ns // 2
    count = PIECES * jnp.maximum(pairs - 1 - sec // 2, 0) // pairs if pairs else 0 * sec
    return jnp.where((sec % 2 == 1) & (sec + 1 < ns), count, 0)


def kernel(
    n, ns,
    slot_ref, stash_ref, doc_hbm, gain_hbm, cos_hbm, sin_hbm, wq_ref, wk_ref, wv_ref,
    q, k, v, dcol, drow,
    raw, mine, dmine, w, xbuf, zbuf, dbuf, acc,
    raw_sem, w_sem, shift_send, right_send, left_send, recv,
    zright_send, zleft_send, zrecv,
    dshift_send, dright_send, dleft_send, drecv,
    doc_ref, gain_ref, cos_ref, sin_ref, small_sem,
):
    me = lax.axis_index("tp")
    sec = lax.axis_index("section")
    slots, rows, width = raw.shape
    pieces = PIECES
    part = width // pieces
    nq, nk = wq_ref.shape[1], wk_ref.shape[1]
    total_n = w.shape[2]
    total = n * rows
    has_right, has_left = me + 1 < n, me > 0
    has_next, has_prev = sec + 1 < ns, sec > 0
    early, early_prev = early_pieces(sec, ns), early_pieces(sec - 1, ns)

    raw_copy = pltpu.make_async_copy(stash_ref.at[0], raw, raw_sem)
    raw_copy.start()
    small = [
        pltpu.make_async_copy(src, dst, small_sem.at[i])
        for i, (src, dst) in enumerate(
            ((gain_hbm, gain_ref), (doc_hbm, doc_ref), (cos_hbm, cos_ref), (sin_hbm, sin_ref))
        )
    ]
    for c in small:
        c.start()

    bar = pltpu.get_barrier_semaphore()
    for cond, target in (
        (has_right, {"tp": me + 1}),
        (has_left, {"tp": me - 1}),
        (has_next, {"section": sec + 1}),
        (has_prev, {"section": sec - 1}),
    ):
        @pl.when(cond)
        def _():
            pl.semaphore_signal(bar, inc=1, device_id=target, device_id_type=MESH)

    def w_copies(p):
        span = pl.ds(pl.multiple_of(p * part, part), part)
        return (
            pltpu.make_async_copy(wq_ref.at[span], w.at[p, :, 0:nq], w_sem.at[p, 0]),
            pltpu.make_async_copy(wk_ref.at[span], w.at[p, :, nq:nq + nk], w_sem.at[p, 1]),
            pltpu.make_async_copy(wv_ref.at[span], w.at[p, :, nq + nk:total_n], w_sem.at[p, 2]),
        )

    @pl.when(has_prev)
    def _():
        for p in range(pieces):
            for c in w_copies(p):
                c.start()

    chosen = slot_ref[0]
    dmine[...] = jnp.zeros_like(dmine)
    for c in small:
        c.wait()
    docs = doc_ref[0, 0:1, :]
    for i in range(1, slots):
        docs = jnp.where(jnp.full(docs.shape, chosen, jnp.int32) == i, doc_ref[0, i:i + 1, :], docs)
    dmine[0:1, 0:rows] = docs
    raw_copy.wait()
    step = 16
    for r in range(0, rows, step):
        x = raw[0, r:r + step, :]
        for i in range(1, slots):
            x = jnp.where(jnp.full(x.shape, chosen, jnp.int32) == i, raw[i, r:r + step, :], x)
        x = x.astype(jnp.float32)
        scale = lax.rsqrt(jnp.mean(x * x, axis=-1, keepdims=True) + NORM_EPSILON)
        y = (x * scale * gain_ref[...].astype(jnp.float32)[None, :]).astype(jnp.bfloat16)
        for p in range(pieces):
            mine[p, r:r + step, :] = y[:, p * part:(p + 1) * part]

    def edges(a):
        return a.astype(jnp.int32)

    pl.semaphore_wait(bar, edges(has_right) + edges(has_left) + edges(has_next) + edges(has_prev))

    def remote(src, dst, ss, rs, target):
        return pltpu.make_async_remote_copy(
            src_ref=src, dst_ref=dst, send_sem=ss, recv_sem=rs, device_id=target, device_id_type=MESH
        )

    def hop(src, c, p):
        return remote(src, xbuf.at[c, p], shift_send.at[c, p], recv.at[c, p], {"section": sec + 1})

    def shift(p):
        return hop(mine.at[p], me, p)

    def zright(src, c, p):
        return remote(src, zbuf.at[c, p], zright_send.at[c, p], zrecv.at[c, p], {"tp": me + 1})

    def zleft(src, c, p):
        return remote(src, zbuf.at[c, p], zleft_send.at[c, p], zrecv.at[c, p], {"tp": me - 1})

    def dshift():
        return remote(dmine, dbuf.at[me], dshift_send, drecv.at[me], {"section": sec + 1})

    def right(c, p):
        b = xbuf.at[c, p]
        return remote(b, b, right_send.at[c, p], recv.at[c, p], {"tp": me + 1})

    def left(c, p):
        b = xbuf.at[c, p]
        return remote(b, b, left_send.at[c, p], recv.at[c, p], {"tp": me - 1})

    def dright(c):
        b = dbuf.at[c]
        return remote(b, b, dright_send.at[c], drecv.at[c], {"tp": me + 1})

    def dleft(c):
        b = dbuf.at[c]
        return remote(b, b, dleft_send.at[c], drecv.at[c], {"tp": me - 1})

    @pl.when(has_next)
    def _():
        dshift().start()
        for p in range(pieces):
            shift(p).start()
            for cond, make in ((has_right, zright), (has_left, zleft)):
                @pl.when(cond & (p < early))
                def _():
                    make(mine.at[p], me, p).start()

    tile = 256

    def compute(c, p, last):
        x = xbuf[c, p]
        for t in range(0, total_n, tile):
            acc[c, :, t:t + tile] += jnp.dot(x, w[p, :, t:t + tile], preferred_element_type=jnp.float32)

        if last is False:
            return

        @pl.when(last)
        def _():
            span = pl.ds(pl.multiple_of(c * rows, rows), rows)
            cos, sin = cos_ref[span, :], sin_ref[span, :]
            for h in range(0, nq + nk, HEAD_SIZE):
                u = acc[c, :, h:h + HEAD_SIZE]
                u = (u * cos + pltpu.roll(u, HEAD_SIZE // 2, 1) * sin).astype(jnp.bfloat16)
                if h < nq:
                    q[span, h:h + HEAD_SIZE] = u
                else:
                    k[span, h - nq:h - nq + HEAD_SIZE] = u
            v[span, :] = acc[c, :, nq + nk:total_n].astype(jnp.bfloat16)

    def own_forward():
        @pl.loop(0, pieces)
        def _(p):
            @pl.when(has_right & (p >= early_prev))
            def _():
                right(me, p).start()

            @pl.when(has_left & (p >= early_prev))
            def _():
                left(me, p).start()

    def keep_docs(c):
        drow[c] = dbuf[c]
        lanes = dbuf.shape[2]
        wide = jnp.broadcast_to(dbuf[c, 0:1, :].astype(jnp.float32), (lanes, lanes))
        dcol[pl.ds(pl.multiple_of(c * rows, rows), rows), :] = wide.T[0:rows, :]

    @pl.when(has_prev)
    def _():
        acc[...] = jnp.zeros_like(acc)
        dshift().wait_recv()

        @pl.when(has_right)
        def _():
            dright(me).start()

        @pl.when(has_left)
        def _():
            dleft(me).start()

        keep_docs(me)

        @pl.loop(0, pieces)
        def _(p):
            shift(p).wait_recv()

        own_forward()

        @pl.loop(0, pieces)
        def _(p):
            for c in w_copies(p):
                c.wait()
            compute(me, p, p == pieces - 1)

    def pass_early(d, p):
        below, above = me - d, me + d

        @pl.when(below >= 0)
        def _():
            b = zbuf.at[below, p]
            zright(b, below, p).wait_recv()

            @pl.when(has_right)
            def _():
                zright(b, below, p).start()

            hop(b, below, p).start()

        @pl.when(above < n)
        def _():
            b = zbuf.at[above, p]
            zleft(b, above, p).wait_recv()

            @pl.when(has_left)
            def _():
                zleft(b, above, p).start()

            hop(b, above, p).start()

    def take_early(below, above):
        @pl.loop(0, 2 * pieces)
        def _(i):
            c = jnp.where(i < pieces, below, above)
            p = i % pieces

            @pl.when((c >= 0) & (c < n) & (p < early_prev))
            def _():
                hop(xbuf.at[c, p], c, p).wait_recv()
                compute(c, p, False)

    @pl.when(has_prev)
    def _():
        @pl.loop(0, (n - 1) * pieces)
        def _(i):
            d, p = i // pieces + 1, i % pieces
            below, above = me - d, me + d
            late = p >= early_prev

            @pl.when(p == 0)
            def _():
                @pl.loop(0, pieces)
                def _(e):
                    @pl.when(e < early)
                    def _():
                        pass_early(d, e)

            @pl.when((below >= 0) & (p == 0))
            def _():
                dright(below).wait_recv()

                @pl.when(has_right)
                def _():
                    dright(below).start()

                keep_docs(below)

            @pl.when((above < n) & (p == 0))
            def _():
                dleft(above).wait_recv()

                @pl.when(has_left)
                def _():
                    dleft(above).start()

                keep_docs(above)

            final = p == pieces - 1

            @pl.when(final & (d == n - 1))
            def _():
                take_early(below, above)

            @pl.when(late & (below >= 0))
            def _():
                right(below, p).wait_recv()

                @pl.when(has_right)
                def _():
                    right(below, p).start()

            @pl.when(late & (above < n))
            def _():
                left(above, p).wait_recv()

                @pl.when(has_left)
                def _():
                    left(above, p).start()

            @pl.when(final & (d < n - 1))
            def _():
                take_early(below, above)

            @pl.when(late & (below >= 0))
            def _():
                compute(below, p, final)

            @pl.when(late & (above < n))
            def _():
                compute(above, p, final)

        @pl.loop(0, n * pieces)
        def _(i):
            c, p = i // pieces, i % pieces

            @pl.when(has_right & (c <= me) & (p == 0))
            def _():
                dright(c).wait_send()

            @pl.when(has_left & (c >= me) & (p == 0))
            def _():
                dleft(c).wait_send()

            @pl.when(has_right & (c <= me) & (p >= early_prev))
            def _():
                right(c, p).wait_send()

            @pl.when(has_left & (c >= me) & (p >= early_prev))
            def _():
                left(c, p).wait_send()

    @pl.when(has_next)
    def _():
        dshift().wait_send()

        @pl.loop(0, n * pieces)
        def _(i):
            c, p = i // pieces, i % pieces

            @pl.when((c == me) | (p < early))
            def _():
                hop(zbuf.at[c, p], c, p).wait_send()

            @pl.when(has_right & (c <= me) & (p < early))
            def _():
                zright(zbuf.at[c, p], c, p).wait_send()

            @pl.when(has_left & (c >= me) & (p < early))
            def _():
                zleft(zbuf.at[c, p], c, p).wait_send()


def attend(n, rows, q, k, v, dcol, drow, out_ref, s_buf, p_buf):
    sec = lax.axis_index("section")
    g = pl.program_id(0)
    total = n * rows
    group = out_ref.shape[2] // HEAD_SIZE
    block = 128 if total % 128 == 0 else total
    factor = math.log2(math.e) / math.sqrt(HEAD_SIZE)

    @pl.when(sec == 0)
    def _():
        out_ref[...] = jnp.zeros_like(out_ref)

    @pl.when(sec > 0)
    def _():
        lane_docs = jnp.concatenate([drow[c, 0:1, 0:rows] for c in range(n)], axis=1).astype(jnp.float32)
        cols = pl.ds(pl.multiple_of(g * HEAD_SIZE, HEAD_SIZE), HEAD_SIZE)
        vg = v[:, cols]
        vg = jnp.concatenate([vg, jnp.ones_like(vg)], axis=1)
        starts = range(0, total, block)
        for i in starts:
            upto = i + block
            keys = k[0:upto, cols]
            i_idx = lax.broadcasted_iota(jnp.int32, (block, upto), 0) + i
            j_idx = lax.broadcasted_iota(jnp.int32, (block, upto), 1)
            allowed = (j_idx <= i_idx) & (dcol[i:upto, 0:1] == lane_docs[:, 0:upto])
            for h in range(group):
                wide = pl.ds(pl.multiple_of((g * group + h) * HEAD_SIZE, HEAD_SIZE), HEAD_SIZE)
                raw = lax.dot_general(
                    q[i:upto, wide], keys, (((1,), (1,)), ((), ())), preferred_element_type=jnp.float32
                )
                s_buf[h, i:upto, 0:upto] = jnp.where(allowed, raw, -1e30)
        for i in starts:
            upto = i + block
            for h in range(group):
                x = s_buf[h, i:upto, 0:upto]
                e = jnp.exp2((x - jnp.max(x, axis=-1, keepdims=True)) * factor)
                p_buf[h, i:upto, 0:upto] = e.astype(jnp.bfloat16)
        for i in starts:
            upto = i + block
            for h in range(group):
                both = jnp.dot(p_buf[h, i:upto, 0:upto], vg[0:upto], preferred_element_type=jnp.float32)
                out_ref[0, i:upto, h * HEAD_SIZE:(h + 1) * HEAD_SIZE] = (
                    both[:, 0:HEAD_SIZE] / both[:, HEAD_SIZE:]
                ).astype(jnp.bfloat16)


def per_device(stash, slot, doc_ids, norm_gain, w_query, w_key, value_weight):
    n, ns = lax.axis_size("tp"), lax.axis_size("section")
    _, slots, rows, width = stash.shape
    total = n * rows
    nq, nk = w_query.shape[1], w_key.shape[1]
    total_n = nq + nk + value_weight.shape[1]
    cos, sin = rope_tables(total)
    lanes = -(-rows // 128) * 128
    bf, f32, dma = jnp.bfloat16, jnp.float32, pltpu.SemaphoreType.DMA
    part = width // PIECES
    q, k, v, dcol, drow = pl.pallas_call(
        functools.partial(kernel, n, ns),
        out_shape=(
            jax.ShapeDtypeStruct((total, nq), bf),
            jax.ShapeDtypeStruct((total, nk), bf),
            jax.ShapeDtypeStruct((total, nk), bf),
            jax.ShapeDtypeStruct((total, lanes), f32),
            jax.ShapeDtypeStruct((n, 8, lanes), jnp.int32),
        ),
        in_specs=[pl.BlockSpec(memory_space=pltpu.SMEM)] + [ANY] * 8,
        out_specs=(VMEM,) * 5,
        scratch_shapes=[
            pltpu.VMEM((slots, rows, width), bf),
            pltpu.VMEM((PIECES, rows, part), bf),
            pltpu.VMEM((8, lanes), jnp.int32),
            pltpu.VMEM((PIECES, part, total_n), bf),
            pltpu.VMEM((n, PIECES, rows, part), bf),
            pltpu.VMEM((n, PIECES, rows, part), bf),
            pltpu.VMEM((n, 8, lanes), jnp.int32),
            pltpu.VMEM((n, rows, total_n), f32),
            dma,
            dma((PIECES, 3)),
            dma((n, PIECES)),
            dma((n, PIECES)),
            dma((n, PIECES)),
            dma((n, PIECES)),
            dma((n, PIECES)),
            dma((n, PIECES)),
            dma((n, PIECES)),
            dma,
            dma((n,)),
            dma((n,)),
            dma((n,)),
            pltpu.VMEM(doc_ids.shape, jnp.int32),
            pltpu.VMEM(norm_gain.shape, bf),
            pltpu.VMEM(cos.shape, f32),
            pltpu.VMEM(sin.shape, f32),
            dma((4,)),
        ],
        compiler_params=pltpu.CompilerParams(
            collective_id=0, has_side_effects=True, vmem_limit_bytes=GATHER_VMEM
        ),
        cost_estimate=pl.CostEstimate(
            flops=2 * total * width * total_n, bytes_accessed=width * total_n * 2, transcendentals=0
        ),
    )(slot, stash, doc_ids, norm_gain, cos, sin, w_query, w_key, value_weight)
    heads = nk // HEAD_SIZE
    return pl.pallas_call(
        functools.partial(attend, n, rows),
        grid=(heads,),
        out_shape=jax.ShapeDtypeStruct((1, total, nq), bf),
        in_specs=[VMEM] * 5,
        out_specs=pl.BlockSpec((1, total, nq // heads), lambda g: (0, 0, g)),
        scratch_shapes=[
            pltpu.VMEM((nq // nk, total, total), f32),
            pltpu.VMEM((nq // nk, total, total), bf),
        ],
        compiler_params=pltpu.CompilerParams(vmem_limit_bytes=ATTEND_VMEM),
    )(q, k, v, dcol, drow)


def solution(mesh):
    placed = (
        P("section", None, "tp", None),
        P("section"),
        P("section", None, "tp"),
        P(),
        P(None, "tp"),
        P(None, "tp"),
        P(None, "tp"),
    )
    return jax.shard_map(
        per_device, mesh=mesh, in_specs=placed, out_specs=P("section", None, "tp"), check_vma=False
    )
```
